32 devices in a mesh: section: 16 (over z, y, core), tensor: 2 (over x).
Axes of the slice: x: 2, y: 2, z: 4, core: 2. Of those that a mesh axis runs over, the one named last changes fastest.
Arguments:
- saved: bfloat16 [16, 16, 64, 8192], P('section', None, 'tensor'), may hold values from -6 to 6
- offsets: int32 [16, 16], P('section'), may hold values from 0 to 15, as said below
Outputs:
- restored: float32 [16, 16, 64, 8192], P('section', None, None, 'tensor')
- block_sums: float32 [16, 16, 8192], P('section', None, 'tensor')
The draws below stay inside these ranges and needn't reach their ends.
Inputs may be any that keep to these rules, and one draw needn't show every extreme that they name: Each row of offsets is a permutation of 0 to 15.
All inputs are finite; a program needn't handle non-finite values.
Results may differ from the reference program's by a relative error of at most 0.0003.
Values may be sent and summed in bfloat16 or wider, within the bound.
No kernel may reach another device: no remote copies, remote signals or barrier semaphores. Data moves between devices by JAX's collectives and lax.ppermute only.
A program may use at most 128 MiB of HBM per device.

```python
import jax
import jax.numpy as jnp

D = 8192
R = 64
SLOTS = 16
N_SECTION = 16


def draw_offsets(key, part):
    row_keys = jax.random.split(jax.random.fold_in(key, 17), N_SECTION)
    rows = jax.vmap(lambda k: jax.random.permutation(k, N_SECTION))(row_keys)
    return rows.astype(jnp.int32)


def shard_levels(stream_key, dims, cuts, least, largest):
    def one(dim, parts):
        draws = jax.random.uniform(jax.random.fold_in(jax.random.fold_in(stream_key, 6), dim), (parts,), jnp.float32, least / len(cuts), largest / len(cuts))
        return jnp.repeat(jnp.exp(draws), dims[dim] // parts).reshape((-1,) + (1,) * (len(dims) - dim - 1))

    factor_of = one(*cuts[0])
    for cut in cuts[1:]:
        factor_of = factor_of * one(*cut)
    return factor_of


def gaussian(stream_key, dims, width, limit, cuts=(), kind=jnp.bfloat16):
    loudness = shard_levels(stream_key, dims, cuts, -0.22, 0.18) if cuts else 1.0
    entries = jax.random.normal(stream_key, dims, jnp.float32) * width * loudness
    return jnp.minimum(jnp.maximum(entries, -limit), limit).astype(kind)


def setup_inputs(seed: int = 0) -> dict:
    keys = jax.random.split(jax.random.key(seed), 3)
    return {
        "saved": gaussian(keys[0], (N_SECTION, SLOTS, R, D), 1.0, 6.0, ((0, 16), (2, 2))),
        "offsets": draw_offsets(jax.random.fold_in(keys[2], 71), 0),
    }


def reference(saved, offsets):
    sections = jnp.arange(N_SECTION, dtype=jnp.int32)
    relative = ((sections[:, None] - sections[None, :]) % N_SECTION).astype(jnp.int32)
    inverse = jnp.argsort(offsets, axis=1).astype(jnp.int32)
    sources = jnp.broadcast_to(sections[None, :], (N_SECTION, N_SECTION)).astype(jnp.int32)
    chosen = inverse[sources, relative]
    blocks = saved[sources, chosen]
    restored = blocks.astype(jnp.float32)
    block_sums = jnp.sum(restored, axis=2)
    return restored, block_sums
```

```python
import jax
import jax.numpy as jnp
from jax import lax
from jax.experimental import pallas as pl
from jax.experimental.pallas import tpu as pltpu
from jax.sharding import PartitionSpec as P


def pack(blocks, target, parts):
    count, rows, cols = blocks.shape
    width = cols // parts

    def kernel(target_ref, in_ref, out_ref):
        for c in range(parts):
            out_ref[0, c] = in_ref[0, :, c * width:(c + 1) * width]

    return pl.pallas_call(
        kernel,
        grid_spec=pltpu.PrefetchScalarGridSpec(
            num_scalar_prefetch=1,
            grid=(count,),
            in_specs=[pl.BlockSpec((1, rows, cols), lambda j, target: (j, 0, 0))],
            out_specs=pl.BlockSpec((1, parts, rows, width), lambda j, target: (target[j], 0, 0, 0)),
        ),
        out_shape=jax.ShapeDtypeStruct((count, parts, rows, width), blocks.dtype),
        name="pack",
    )(target, blocks)


def unpack(arrived):
    count, rows, width = arrived.shape

    def kernel(in_ref, out_ref, sums_ref):
        s = pl.program_id(0)
        block = in_ref[0].astype(jnp.float32)
        out_ref[0, 0] = block
        sums_ref[0, pl.ds(s, 1), :] = jnp.sum(block, axis=0, keepdims=True)

    return pl.pallas_call(
        kernel,
        grid=(count,),
        in_specs=[pl.BlockSpec((1, rows, width), lambda s: (s, 0, 0))],
        out_specs=[
            pl.BlockSpec((1, 1, rows, width), lambda s: (0, s, 0, 0)),
            pl.BlockSpec((1, count, width), lambda s: (0, 0, 0)),
        ],
        out_shape=[
            jax.ShapeDtypeStruct((1, count, rows, width), jnp.float32),
            jax.ShapeDtypeStruct((1, count, width), jnp.float32),
        ],
        name="unpack",
    )(arrived)


def body(saved, offsets):
    count = lax.axis_size("section")
    parts = lax.axis_size("tensor")
    mine = lax.axis_index("section")
    _, _, rows, cols = saved.shape
    target = (mine + offsets[0]) % count
    outgoing = pack(saved[0], target, parts).reshape(count * parts, rows, cols // parts)
    arrived = lax.all_to_all(outgoing, ("section", "tensor"), split_axis=0, concat_axis=0, tiled=True)
    restored, block_sums = unpack(arrived.reshape(count, parts * rows, cols // parts))
    return (restored, block_sums)


def solution(mesh):
    return jax.shard_map(
        body,
        mesh=mesh,
        in_specs=(P("section", None, "tensor", None), P("section", None)),
        out_specs=(P("section", None, None, "tensor"), P("section", None, "tensor")),
        check_vma=False,
    )
```

```python
import jax
import jax.numpy as jnp
from jax import lax
from jax.experimental import pallas as pl
from jax.experimental.pallas import tpu as pltpu
from jax.sharding import PartitionSpec as P

CHUNKS = 4
VMEM = 67043328
ANY = pl.BlockSpec(memory_space=pl.ANY)


def cost(elements):
    return pl.CostEstimate(flops=elements, bytes_accessed=6 * elements, transcendentals=0)


def pack(saved, offsets, distances, parts):
    _, count, rows, cols = saved.shape
    width = cols // parts
    total = len(distances) * parts

    def kernel(offsets_ref, saved_ref, *refs):
        outs, (held, come, go) = refs[:total], refs[total:]
        mine, part = lax.axis_index("section"), lax.axis_index("tensor")
        reads = []
        for i, d in enumerate(distances):
            slot = jnp.int32(0)
            for j in range(count):
                hit = lax.rem(mine + offsets_ref[0, j], count) == (mine ^ d)
                slot = jnp.where(hit, j, slot)
            for x in range(parts):
                n = i * parts + x
                start = pl.multiple_of((part ^ x) * width, width)
                reads.append(
                    pltpu.make_async_copy(
                        saved_ref.at[0, slot, :, pl.ds(start, width)], held.at[n], come.at[n]
                    )
                )
                reads[-1].start()
        writes = []
        for n, read in enumerate(reads):
            read.wait()
            writes.append(pltpu.make_async_copy(held.at[n], outs[n], go.at[n]))
            writes[-1].start()
        for write in writes:
            write.wait()

    pieces = pl.pallas_call(
        kernel,
        in_specs=[pl.BlockSpec(memory_space=pltpu.SMEM), ANY],
        out_specs=[ANY] * total,
        out_shape=[jax.ShapeDtypeStruct((rows, width), saved.dtype)] * total,
        scratch_shapes=[
            pltpu.VMEM((total, rows, width), saved.dtype),
            pltpu.SemaphoreType.DMA((total,)),
            pltpu.SemaphoreType.DMA((total,)),
        ],
        cost_estimate=cost(total * rows * width),
        name="pack",
    )(offsets, saved)
    return {d: list(pieces[i * parts:(i + 1) * parts]) for i, d in enumerate(distances)}


def unpack(pieces, so_far, distance, count):
    parts = len(pieces)
    rows, width = pieces[0].shape
    tile = width // CHUNKS
    first = so_far is None

    def kernel(*refs):
        ins = refs[:parts]
        out_ref, sums_ref, held, wide, sums, come, go, sums_sem = refs[-8:]
        source = lax.axis_index("section") ^ distance
        part = lax.axis_index("tensor")

        def columns(c):
            return pl.ds(c * tile, tile)

        def arrival(c, x):
            return pltpu.make_async_copy(
                ins[x].at[:, columns(c)], held.at[x, :, columns(c)], come.at[c, x]
            )

        def departure(c):
            return pltpu.make_async_copy(
                wide.at[:, columns(c)], out_ref.at[0, source, :, columns(c)], go.at[c]
            )

        for c in range(CHUNKS):
            for x in range(parts):
                arrival(c, x).start()
        if first:
            sums[...] = jnp.zeros_like(sums)
        else:
            load = pltpu.make_async_copy(refs[parts + 1].at[0], sums, sums_sem.at[0])
            load.start()
        for c in range(CHUNKS):
            total = None
            for x in range(parts):
                arrival(c, x).wait()
                start = pl.multiple_of((part ^ x) * rows, rows)
                piece = held[x, :, columns(c)].astype(jnp.float32)
                wide[pl.ds(start, rows), columns(c)] = piece
                some = jnp.sum(piece, axis=0, keepdims=True)
                total = some if total is None else total + some
            departure(c).start()
            if c == 0 and not first:
                load.wait()
            sums[pl.ds(source, 1), columns(c)] = total
        store = pltpu.make_async_copy(sums, sums_ref.at[0], sums_sem.at[1])
        store.start()
        for c in range(CHUNKS):
            departure(c).wait()
        store.wait()

    return pl.pallas_call(
        kernel,
        in_specs=[ANY] * (parts + (0 if first else 2)),
        out_specs=[ANY, ANY],
        out_shape=[
            jax.ShapeDtypeStruct((1, count, parts * rows, width), jnp.float32),
            jax.ShapeDtypeStruct((1, count, width), jnp.float32),
        ],
        scratch_shapes=[
            pltpu.VMEM((parts, rows, width), pieces[0].dtype),
            pltpu.VMEM((parts * rows, width), jnp.float32),
            pltpu.VMEM((count, width), jnp.float32),
            pltpu.SemaphoreType.DMA((CHUNKS, parts)),
            pltpu.SemaphoreType.DMA((CHUNKS,)),
            pltpu.SemaphoreType.DMA((2,)),
        ],
        input_output_aliases={} if first else {parts: 0, parts + 1: 1},
        cost_estimate=cost(parts * rows * width),
        compiler_params=pltpu.CompilerParams(vmem_limit_bytes=VMEM),
        name="unpack",
    )(*pieces, *(() if first else so_far))


def by_permutes(saved, offsets):
    count = lax.axis_size("section")
    parts = lax.axis_size("tensor")
    half = count // 2
    issue = [
        (d, x) for pair in zip(range(half, count), range(half)) for d in pair for x in range(parts)
    ]
    finish = [p[0] for i, p in enumerate(issue) if p[0] not in [q[0] for q in issue[i + 1:]]]
    arrived = pack(saved, offsets, [half], parts)
    arrived.update(pack(saved, offsets, [d for d in range(count) if d != half], parts))
    for d, x in issue:
        if d or x:
            pairs = [
                (s * parts + t, (s ^ d) * parts + (t ^ x))
                for s in range(count)
                for t in range(parts)
            ]
            arrived[d][x] = lax.ppermute(arrived[d][x], ("section", "tensor"), pairs)
    so_far = None
    for d in finish:
        so_far = unpack(arrived[d], so_far, d, count)
    return tuple(so_far)


def pack_all(blocks, target, parts):
    count, rows, cols = blocks.shape
    width = cols // parts

    def kernel(target_ref, in_ref, out_ref):
        for c in range(parts):
            out_ref[0, c] = in_ref[0, :, c * width:(c + 1) * width]

    return pl.pallas_call(
        kernel,
        grid_spec=pltpu.PrefetchScalarGridSpec(
            num_scalar_prefetch=1,
            grid=(count,),
            in_specs=[pl.BlockSpec((1, rows, cols), lambda j, target: (j, 0, 0))],
            out_specs=pl.BlockSpec((1, parts, rows, width), lambda j, target: (target[j], 0, 0, 0)),
        ),
        out_shape=jax.ShapeDtypeStruct((count, parts, rows, width), blocks.dtype),
        name="pack",
    )(target, blocks)


def unpack_all(arrived):
    count, rows, width = arrived.shape

    def kernel(in_ref, out_ref, sums_ref):
        s = pl.program_id(0)
        block = in_ref[0].astype(jnp.float32)
        out_ref[0, 0] = block
        sums_ref[0, pl.ds(s, 1), :] = jnp.sum(block, axis=0, keepdims=True)

    return pl.pallas_call(
        kernel,
        grid=(count,),
        in_specs=[pl.BlockSpec((1, rows, width), lambda s: (s, 0, 0))],
        out_specs=[
            pl.BlockSpec((1, 1, rows, width), lambda s: (0, s, 0, 0)),
            pl.BlockSpec((1, count, width), lambda s: (0, 0, 0)),
        ],
        out_shape=[
            jax.ShapeDtypeStruct((1, count, rows, width), jnp.float32),
            jax.ShapeDtypeStruct((1, count, width), jnp.float32),
        ],
        name="unpack",
    )(arrived)


def by_all_to_all(saved, offsets):
    count = lax.axis_size("section")
    parts = lax.axis_size("tensor")
    mine = lax.axis_index("section")
    _, _, rows, cols = saved.shape
    target = (mine + offsets[0]) % count
    outgoing = pack_all(saved[0], target, parts).reshape(count * parts, rows, cols // parts)
    arrived = lax.all_to_all(outgoing, ("section", "tensor"), split_axis=0, concat_axis=0, tiled=True)
    restored, block_sums = unpack_all(arrived.reshape(count, parts * rows, cols // parts))
    return (restored, block_sums)


def solution(mesh):
    sizes = (mesh.shape["section"], mesh.shape["tensor"])
    even = all(n > 1 and n & (n - 1) == 0 for n in sizes)
    few = sizes[0] * sizes[1] <= 32
    return jax.shard_map(
        by_permutes if even and few else by_all_to_all,
        mesh=mesh,
        in_specs=(P("section", None, "tensor", None), P("section", None)),
        out_specs=(P("section", None, None, "tensor"), P("section", None, "tensor")),
        check_vma=False,
    )
```

```python
import jax
import jax.numpy as jnp
from jax import lax
from jax.experimental import pallas as pl
from jax.experimental.pallas import tpu as pltpu
from jax.sharding import PartitionSpec as P

CHUNKS = 2
VMEM = 67043328
ANY = pl.BlockSpec(memory_space=pl.ANY)


def cost(elements):
    return pl.CostEstimate(flops=elements, bytes_accessed=6 * elements, transcendentals=0)


def pack(saved, offsets, distances, parts):
    _, count, rows, cols = saved.shape
    width = cols // parts
    total = len(distances) * parts

    def kernel(offsets_ref, saved_ref, *refs):
        outs, (held, come, go) = refs[:total], refs[total:]
        mine, part = lax.axis_index("section"), lax.axis_index("tensor")
        reads = []
        for i, d in enumerate(distances):
            slot = jnp.int32(0)
            for j in range(count):
                hit = lax.rem(mine + offsets_ref[0, j], count) == (mine ^ d)
                slot = jnp.where(hit, j, slot)
            for x in range(parts):
                n = i * parts + x
                start = pl.multiple_of((part ^ x) * width, width)
                reads.append(
                    pltpu.make_async_copy(
                        saved_ref.at[0, slot, :, pl.ds(start, width)], held.at[n], come.at[n]
                    )
                )
                reads[-1].start()
        writes = []
        for n, read in enumerate(reads):
            read.wait()
            writes.append(pltpu.make_async_copy(held.at[n], outs[n], go.at[n]))
            writes[-1].start()
        for write in writes:
            write.wait()

    pieces = pl.pallas_call(
        kernel,
        in_specs=[pl.BlockSpec(memory_space=pltpu.SMEM), ANY],
        out_specs=[ANY] * total,
        out_shape=[jax.ShapeDtypeStruct((rows, width), saved.dtype)] * total,
        scratch_shapes=[
            pltpu.VMEM((total, rows, width), saved.dtype),
            pltpu.SemaphoreType.DMA((total,)),
            pltpu.SemaphoreType.DMA((total,)),
        ],
        cost_estimate=cost(total * rows * width),
        name="pack",
    )(offsets, saved)
    return {d: list(pieces[i * parts:(i + 1) * parts]) for i, d in enumerate(distances)}


def unpack(pieces, so_far, distance, count):
    parts = len(pieces)
    rows, width = pieces[0].shape
    tile = width // CHUNKS
    first = so_far is None

    def kernel(*refs):
        ins = refs[:parts]
        out_ref, sums_ref, held, wide, sums, come, go, sums_sem = refs[-8:]
        source = lax.axis_index("section") ^ distance
        part = lax.axis_index("tensor")

        def columns(c):
            return pl.ds(c * tile, tile)

        def arrival(c, x):
            return pltpu.make_async_copy(
                ins[x].at[:, columns(c)], held.at[x, :, columns(c)], come.at[c, x]
            )

        def departure(c):
            return pltpu.make_async_copy(
                wide.at[:, columns(c)], out_ref.at[0, source, :, columns(c)], go.at[c]
            )

        for c in range(CHUNKS):
            for x in range(parts):
                arrival(c, x).start()
        if first:
            sums[...] = jnp.zeros_like(sums)
        else:
            load = pltpu.make_async_copy(refs[parts + 1].at[0], sums, sums_sem.at[0])
            load.start()
        for c in range(CHUNKS):
            total = None
            for x in range(parts):
                arrival(c, x).wait()
                start = pl.multiple_of((part ^ x) * rows, rows)
                piece = held[x, :, columns(c)].astype(jnp.float32)
                wide[pl.ds(start, rows), columns(c)] = piece
                some = jnp.sum(piece, axis=0, keepdims=True)
                total = some if total is None else total + some
            departure(c).start()
            if c == 0 and not first:
                load.wait()
            sums[pl.ds(source, 1), columns(c)] = total
        store = pltpu.make_async_copy(sums, sums_ref.at[0], sums_sem.at[1])
        store.start()
        for c in range(CHUNKS):
            departure(c).wait()
        store.wait()

    return pl.pallas_call(
        kernel,
        in_specs=[ANY] * (parts + (0 if first else 2)),
        out_specs=[ANY, ANY],
        out_shape=[
            jax.ShapeDtypeStruct((1, count, parts * rows, width), jnp.float32),
            jax.ShapeDtypeStruct((1, count, width), jnp.float32),
        ],
        scratch_shapes=[
            pltpu.VMEM((parts, rows, width), pieces[0].dtype),
            pltpu.VMEM((parts * rows, width), jnp.float32),
            pltpu.VMEM((count, width), jnp.float32),
            pltpu.SemaphoreType.DMA((CHUNKS, parts)),
            pltpu.SemaphoreType.DMA((CHUNKS,)),
            pltpu.SemaphoreType.DMA((2,)),
        ],
        input_output_aliases={} if first else {parts: 0, parts + 1: 1},
        cost_estimate=cost(parts * rows * width),
        compiler_params=pltpu.CompilerParams(vmem_limit_bytes=VMEM),
        name="unpack",
    )(*pieces, *(() if first else so_far))


def by_permutes(saved, offsets):
    count = lax.axis_size("section")
    parts = lax.axis_size("tensor")
    half = count // 2
    order = [half, 0] + [d for pair in zip(range(1, half), range(half + 1, count)) for d in pair]
    issue = [(d, x) for d in order for x in range(parts)]
    finish = [p[0] for i, p in enumerate(issue) if p[0] not in [q[0] for q in issue[i + 1:]]]
    arrived = pack(saved, offsets, [half], parts)
    arrived.update(pack(saved, offsets, [d for d in range(count) if d != half], parts))
    for d, x in issue:
        if d or x:
            pairs = [
                (s * parts + t, (s ^ d) * parts + (t ^ x))
                for s in range(count)
                for t in range(parts)
            ]
            arrived[d][x] = lax.ppermute(arrived[d][x], ("section", "tensor"), pairs)
    so_far = None
    for d in finish:
        so_far = unpack(arrived[d], so_far, d, count)
    return tuple(so_far)


def pack_all(blocks, target, parts):
    count, rows, cols = blocks.shape
    width = cols // parts

    def kernel(target_ref, in_ref, out_ref):
        for c in range(parts):
            out_ref[0, c] = in_ref[0, :, c * width:(c + 1) * width]

    return pl.pallas_call(
        kernel,
        grid_spec=pltpu.PrefetchScalarGridSpec(
            num_scalar_prefetch=1,
            grid=(count,),
            in_specs=[pl.BlockSpec((1, rows, cols), lambda j, target: (j, 0, 0))],
            out_specs=pl.BlockSpec((1, parts, rows, width), lambda j, target: (target[j], 0, 0, 0)),
        ),
        out_shape=jax.ShapeDtypeStruct((count, parts, rows, width), blocks.dtype),
        name="pack",
    )(target, blocks)


def unpack_all(arrived):
    count, rows, width = arrived.shape

    def kernel(in_ref, out_ref, sums_ref):
        s = pl.program_id(0)
        block = in_ref[0].astype(jnp.float32)
        out_ref[0, 0] = block
        sums_ref[0, pl.ds(s, 1), :] = jnp.sum(block, axis=0, keepdims=True)

    return pl.pallas_call(
        kernel,
        grid=(count,),
        in_specs=[pl.BlockSpec((1, rows, width), lambda s: (s, 0, 0))],
        out_specs=[
            pl.BlockSpec((1, 1, rows, width), lambda s: (0, s, 0, 0)),
            pl.BlockSpec((1, count, width), lambda s: (0, 0, 0)),
        ],
        out_shape=[
            jax.ShapeDtypeStruct((1, count, rows, width), jnp.float32),
            jax.ShapeDtypeStruct((1, count, width), jnp.float32),
        ],
        name="unpack",
    )(arrived)


def by_all_to_all(saved, offsets):
    count = lax.axis_size("section")
    parts = lax.axis_size("tensor")
    mine = lax.axis_index("section")
    _, _, rows, cols = saved.shape
    target = (mine + offsets[0]) % count
    outgoing = pack_all(saved[0], target, parts).reshape(count * parts, rows, cols // parts)
    arrived = lax.all_to_all(outgoing, ("section", "tensor"), split_axis=0, concat_axis=0, tiled=True)
    restored, block_sums = unpack_all(arrived.reshape(count, parts * rows, cols // parts))
    return (restored, block_sums)


def solution(mesh):
    sizes = (mesh.shape["section"], mesh.shape["tensor"])
    even = all(n > 1 and n & (n - 1) == 0 for n in sizes)
    few = sizes[0] * sizes[1] <= 32
    return jax.shard_map(
        by_permutes if even and few else by_all_to_all,
        mesh=mesh,
        in_specs=(P("section", None, "tensor", None), P("section", None)),
        out_specs=(P("section", None, None, "tensor"), P("section", None, "tensor")),
        check_vma=False,
    )
```
